128 devices in a mesh: py: 4 (over y), px: 8 (over z_lo, x), pz: 4 (over z_hi, core).
Axes of the slice: x: 4, y: 4, z: 4 (z_hi: 2, z_lo: 2; z = z_hi * 2 + z_lo), core: 2. Of those that a mesh axis runs over, the one named last changes fastest.
Arguments:
- starting_state: float32 [512, 32, 128, 128], P('py', 'px', 'pz'), may hold values from 0.5 to 2
- scaled_conductivity: float32 [512, 32, 128, 128], P('py', 'px', 'pz'), may hold values from 0.03 to 0.15
- scaled_heat_supply: float32 [512, 32, 128, 128], P('py', 'px', 'pz'), may hold values from -0.2 to 0.2
Outputs:
- normalised_result: float32 [512, 32, 128, 128], P('py', 'px', 'pz')
- temperature_end: float32 [512, 32, 128, 128], P('py', 'px', 'pz')
The draws below stay inside these ranges and needn't reach their ends.
All inputs are finite; a program needn't handle non-finite values.
Results may differ from the reference program's by a relative error of at most 0.00002.
Values sent between devices are 32-bit elements; how exact they have to be, the bound alone decides.
No kernel may reach another device: no remote copies, remote signals or barrier semaphores. Data moves between devices by JAX's collectives and lax.ppermute only.
A program may use at most 128 MiB of HBM per device.

```python
import jax
import jax.numpy as jnp
from jax import lax

GRID_DEPTH = 512
GRID_WIDTH = 32
GRID_HEIGHT = 128
SAMPLE_TOTAL = 128
STEPS = 4


def block_levels(rng, shape, split, low, high):
    def one(position, parts):
        heights = jax.random.uniform(jax.random.fold_in(jax.random.fold_in(rng, 6), position), (parts,), jnp.float32, low / len(split), high / len(split))
        return jnp.repeat(jnp.exp(heights), shape[position] // parts).reshape((-1,) + (1,) * (len(shape) - position - 1))

    level = one(*split[0])
    for cut in split[1:]:
        level = level * one(*cut)
    return level


def setup_inputs(seed: int = 0) -> dict:
    keys = jax.random.split(jax.random.key(seed), 4)
    return {
        "starting_state": jnp.clip(0.5 + 1.5 * jax.random.uniform(keys[0], (GRID_DEPTH, GRID_WIDTH, GRID_HEIGHT, SAMPLE_TOTAL), jnp.float32) ** block_levels(keys[0], (GRID_DEPTH, GRID_WIDTH, GRID_HEIGHT, SAMPLE_TOTAL), ((0, 4), (1, 8), (2, 4)), -0.2, 0.2), 0.5, 2.0),
        "scaled_conductivity": jnp.clip(0.03 + 0.120000007 * jax.random.uniform(keys[1], (GRID_DEPTH, GRID_WIDTH, GRID_HEIGHT, SAMPLE_TOTAL), jnp.float32) ** block_levels(keys[1], (GRID_DEPTH, GRID_WIDTH, GRID_HEIGHT, SAMPLE_TOTAL), ((0, 4), (1, 8), (2, 4)), -0.2, 0.2), 0.03, 0.15),
        "scaled_heat_supply": jnp.clip(jax.random.uniform(keys[2], (GRID_DEPTH, GRID_WIDTH, GRID_HEIGHT, SAMPLE_TOTAL), jnp.float32, -0.2, 0.2) * block_levels(keys[2], (GRID_DEPTH, GRID_WIDTH, GRID_HEIGHT, SAMPLE_TOTAL), ((0, 4), (1, 8), (2, 4)), -0.4, 0.0), -0.2, 0.2),
    }


def interior_points(values, dims):
    for coordinate_axis in dims:
        values = lax.slice_in_dim(values, 1, values.shape[coordinate_axis] - 1, axis=coordinate_axis)
    return values

def boundary_layer(values, coordinate_axis, start, dims):
    others = [other for other in dims if other != coordinate_axis]
    values = interior_points(values, others)
    return lax.slice_in_dim(values, start, start + values.shape[coordinate_axis] - 2, axis=coordinate_axis)

def conduction_timestep(framed_thermal_lattice, scaled_conductivity, scaled_heat_supply):
    central_point = interior_points(framed_thermal_lattice, (0, 1, 2))
    preceding_neighbour = [boundary_layer(framed_thermal_lattice, coordinate_axis, 0, (0, 1, 2)) for coordinate_axis in (0, 1, 2)]
    following_neighbour = [boundary_layer(framed_thermal_lattice, coordinate_axis, 2, (0, 1, 2)) for coordinate_axis in (0, 1, 2)]
    spread = preceding_neighbour[0] + following_neighbour[0] + preceding_neighbour[1] + following_neighbour[1] + preceding_neighbour[2] + following_neighbour[2] - 6.0 * central_point
    return central_point + scaled_conductivity * spread + scaled_heat_supply

def reference(starting_state, scaled_conductivity, scaled_heat_supply):
    for step in range(STEPS):
        starting_state = conduction_timestep(jnp.pad(starting_state, ((1, 1), (1, 1), (1, 1), (0, 0)), mode='constant'), scaled_conductivity, scaled_heat_supply)
    row_average = lax.optimization_barrier(jnp.mean(starting_state, axis=1, keepdims=True))
    deviation_rows = starting_state - row_average
    line_variance = lax.optimization_barrier(jnp.mean(deviation_rows * deviation_rows, axis=1, keepdims=True))
    normalised_result = deviation_rows * lax.rsqrt(line_variance + 0.0001)
    return (normalised_result, starting_state)
```

```python
import functools

import jax
import jax.numpy as jnp
from jax import lax
from jax.experimental import pallas as pl
from jax.experimental.pallas import tpu as pltpu
from jax.sharding import PartitionSpec as P


STEPS = 4


def ring(value, axis, shift):
    devices = lax.axis_size(axis)
    return lax.ppermute(value, axis, [(i, (i + shift) % devices) for i in range(devices)])


def send_up(value, axis):
    return ring(value, axis, 1)


def send_down(value, axis):
    return ring(value, axis, -1)


def swap(value, mask):
    return lax.ppermute(value, "px", [(i, i ^ mask) for i in range(lax.axis_size("px"))])


def pair_swap(value, axis, odd):
    devices = lax.axis_size(axis)
    return lax.ppermute(value, axis, [(i, ((i - odd) ^ 1) + odd) for i in range(odd, devices - odd)])


def exchange(faces, axis):
    even = pair_swap(faces[0], axis, 0)
    odd = pair_swap(faces[1], axis, 1)
    return even, odd


def z_exchange(faces):
    last_x, last_z = lax.axis_size("px") - 1, lax.axis_size("pz") - 1
    flat = lambda x, z: x * (last_z + 1) + z
    direct = [(flat(x, a), flat(x, b)) for x in range(1, last_x) for a, b in ((1, 2), (2, 1))]
    out, back = [], []
    for x, over in ((0, last_x // 2 + 1), (last_x, last_x // 2)):
        out += [(flat(x, 1), flat(over, last_z)), (flat(x, 2), flat(over, 0))]
        back += [(flat(over, last_z), flat(x, 2)), (flat(over, 0), flat(x, 1))]
    even = pair_swap(faces[0], "pz", 0)
    odd = lax.ppermute(faces[1], ("px", "pz"), direct + out)
    over = lax.ppermute(odd, ("px", "pz"), back)
    return even, odd, over


def by_parity(axis, low, high):
    even = lax.axis_index(axis) % 2 == 0
    return jnp.where(even, high, low), jnp.where(even, low, high)


def inside(axis):
    at = lax.axis_index(axis)
    below = jnp.where(at > 0, 1.0, 0.0).astype(jnp.float32)
    above = jnp.where(at < lax.axis_size(axis) - 1, 1.0, 0.0).astype(jnp.float32)
    return below, above


def update_rows(refs, store, block, width, height, is_first, is_last, outer):
    u, before, after, low, high, xe, xo, ze, zo, zo_over, k, s = refs
    x_at, z_at = lax.axis_index("px"), lax.axis_index("pz")
    x_outer = (x_at == 0) | (x_at == lax.axis_size("px") - 1)
    z_inner = ((z_at > 0) & (z_at < lax.axis_size("pz") - 1)).astype(jnp.float32)
    x_even = lax.axis_index("px") % 2 == 0
    z_even = lax.axis_index("pz") % 2 == 0
    y_below, y_above = inside("py")
    sub = lax.broadcasted_iota(jnp.int32, (height, u.shape[-1]), 0)
    at_low = sub == 0
    at_high = sub == height - 1

    def one_row(r, below, above):
        for x in range(width):
            c = u[r, x]
            left = jnp.where(x_even, xo[r], xe[r]) if x == 0 else u[r, x - 1]
            right = jnp.where(x_even, xe[r], xo[r]) if x == width - 1 else u[r, x + 1]
            line = r * width + x
            z_first = ze[pl.ds(line, 1), :]
            z_second = jnp.where(x_outer, zo_over[pl.ds(line, 1), :], zo[pl.ds(line, 1), :]) * z_inner
            zd = jnp.where(at_low, jnp.where(z_even, z_second, z_first), pltpu.roll(c, 1, 0))
            zu = jnp.where(at_high, jnp.where(z_even, z_first, z_second), pltpu.roll(c, height - 1, 0))
            spread = below(x) + above(x) + left + right + zd + zu - 6.0 * c
            store(r, x, c + k[r, x] * spread + s[r, x])

    def lowest(x):
        return jnp.where(is_first, low[0, x] * y_below if outer[0] else low[0, x], before[0, x])

    def highest(x):
        return jnp.where(is_last, high[0, x] * y_above if outer[1] else high[0, x], after[0, x])

    one_row(0, lowest, lambda x: u[1, x])

    def middle(r, carry):
        one_row(r, lambda x: u[r - 1, x], lambda x: u[r + 1, x])
        return carry

    lax.fori_loop(1, block - 1, middle, 0)
    one_row(block - 1, lambda x: u[block - 2, x], highest)


def pick_body(low, high, even_face, odd_face):
    even_face[...], odd_face[...] = by_parity("px", low[:, 0], high[:, 0])


def pick(u, row0, count):
    _, width, height, lanes = u.shape
    block = min(16, count)
    first = row0 // block
    face = jax.ShapeDtypeStruct((count, height, lanes), jnp.float32)
    return pl.pallas_call(
        pick_body,
        grid=(count // block,),
        in_specs=[
            pl.BlockSpec((block, 1, height, lanes), lambda i: (first + i, 0, 0, 0)),
            pl.BlockSpec((block, 1, height, lanes), lambda i: (first + i, width - 1, 0, 0)),
        ],
        out_specs=[pl.BlockSpec((block, height, lanes), lambda i: (i, 0, 0))] * 2,
        out_shape=[face, face],
        compiler_params=pltpu.CompilerParams(dimension_semantics=("arbitrary",)),
        name="pick",
    )(u, u)


def step_body(*refs, block, blocks, extra, y_face, outer):
    ins, outs = refs[:12], refs[12 + extra :]
    width, height = ins[0].shape[1:3]
    i = pl.program_id(0)
    kept = {}

    def store(r, x, value):
        outs[0][r, x] = value
        if x == 0:
            kept["low"] = value
        if x == width - 1:
            outs[3][r], outs[4][r] = by_parity("px", kept["low"], value)
        line = pl.ds(r * width + x, 1)
        outs[1][line, :], outs[2][line, :] = by_parity("pz", value[0:1], value[height - 1 : height])

    update_rows(ins, store, block, width, height, i == 0, i == blocks - 1, outer)
    if y_face == "low":

        @pl.when(i == 0)
        def _():
            outs[5][0] = outs[0][0]

    if y_face == "high":

        @pl.when(i == blocks - 1)
        def _():
            outs[5][0] = outs[0][block - 1]


def field_specs(row0, offset, rows, block, width, height, lanes, low, high, at):
    full = (block, width, height, lanes)
    one = (1, width, height, lanes)
    first = row0 // block
    extra = offset // block
    return [
        pl.BlockSpec(full, lambda *g: (first + at(*g), 0, 0, 0)),
        pl.BlockSpec(one, lambda *g: (jnp.maximum(row0 + at(*g) * block - 1, 0), 0, 0, 0)),
        pl.BlockSpec(one, lambda *g: (jnp.minimum(row0 + (at(*g) + 1) * block, rows - 1), 0, 0, 0)),
        pl.BlockSpec(one, lambda *g: (low, 0, 0, 0)),
        pl.BlockSpec(one, lambda *g: (high, 0, 0, 0)),
        pl.BlockSpec((block, height, lanes), lambda *g: (extra + at(*g), 0, 0)),
        pl.BlockSpec((block, height, lanes), lambda *g: (extra + at(*g), 0, 0)),
        pl.BlockSpec((block * width, lanes), lambda *g: (first + at(*g), 0)),
        pl.BlockSpec((block * width, lanes), lambda *g: (first + at(*g), 0)),
        pl.BlockSpec((block * width, lanes), lambda *g: (first + at(*g), 0)),
        pl.BlockSpec(full, lambda *g: (first + at(*g), 0, 0, 0)),
        pl.BlockSpec(full, lambda *g: (first + at(*g), 0, 0, 0)),
    ]


def advance(u, halos, low, high, k, s, row0, count, offset, targets, block):
    rows, width, height, lanes = u.shape
    block = min(block, count)
    blocks = count // block
    first = row0 // block
    y_face = "low" if row0 == 0 else "high" if row0 + count == rows else None
    specs = field_specs(row0, offset, rows, block, width, height, lanes, low[1], high[1], lambda i: i)
    operands = [u, u, u, low[0], high[0], *halos, k, s]
    aliases = {}
    for number, target in enumerate(targets):
        aliases[len(operands)] = number
        operands.append(target)
        specs.append(pl.BlockSpec(memory_space=pl.ANY))
    face = pl.BlockSpec((block, height, lanes), lambda i: (i, 0, 0))
    edge = pl.BlockSpec((block * width, lanes), lambda i: (first + i, 0))
    out_specs = [pl.BlockSpec((block, width, height, lanes), lambda i: (first + i, 0, 0, 0)), edge, edge, face, face]
    shapes = [u.shape] + [(rows * width, lanes)] * 2 + [(count, height, lanes)] * 2
    if y_face:
        out_specs.append(pl.BlockSpec((1, width, height, lanes), lambda i: (0, 0, 0, 0)))
        shapes.append((1, width, height, lanes))
    return pl.pallas_call(
        functools.partial(
            step_body,
            block=block,
            blocks=blocks,
            extra=len(targets),
            y_face=y_face,
            outer=(row0 == 0, row0 + count == rows),
        ),
        grid=(blocks,),
        in_specs=specs,
        out_specs=out_specs,
        out_shape=[jax.ShapeDtypeStruct(shape, jnp.float32) for shape in shapes],
        input_output_aliases=aliases,
        compiler_params=pltpu.CompilerParams(dimension_semantics=("arbitrary",)),
        name="advance",
    )(*operands)


def final_body(bits, *refs, block, per_part, extra, outer):
    ins, outs = refs[:12], refs[12 + extra :]
    width, height = ins[0].shape[1:3]
    p, i = pl.program_id(0), pl.program_id(1)
    at = jnp.where(p == 0, 1 - bits[0], bits[0]) * per_part + i
    result, send, keep = outs
    totals = {}

    def stats_to(target):
        def store(r, x, value):
            result[r, x] = value
            moved = value - 1.0
            totals["sum"] = moved if x == 0 else totals["sum"] + moved
            totals["square"] = moved * moved if x == 0 else totals["square"] + moved * moved
            if x == width - 1:
                target[0, r] = totals["sum"]
                target[1, r] = totals["square"]

        update_rows(ins, store, block, width, height, at == 0, at == 2 * per_part - 1, outer)

    @pl.when(p == 0)
    def _():
        stats_to(send)

    @pl.when(p == 1)
    def _():
        stats_to(keep)


def finish(u, halos, low, high, k, s, row0, count, offset, target, after, bits, block):
    rows, width, height, lanes = u.shape
    block = min(block, count // 2)
    per_part = count // 2 // block
    first = row0 // block

    def at(p, i, bits):
        return jnp.where(p == 0, 1 - bits[0], bits[0]) * per_part + i

    specs = field_specs(row0, offset, rows, block, width, height, lanes, low[1], high[1], at)
    operands = [bits, u, u, u, low[0], high[0], *halos, k, s]
    aliases = {}
    extra = list(after)
    if target is not None:
        aliases = {len(operands) + len(extra): 0}
        extra.append(target)
    operands += extra
    specs += [pl.BlockSpec(memory_space=pl.ANY)] * len(extra)
    part = (2, block, height, lanes)
    out_specs = [
        pl.BlockSpec((block, width, height, lanes), lambda *g: (first + at(*g), 0, 0, 0)),
        pl.BlockSpec(part, lambda p, i, m: (0, jnp.where(p == 0, i, per_part - 1), 0, 0)),
        pl.BlockSpec(part, lambda p, i, m: (0, jnp.where(p == 0, 0, i), 0, 0)),
    ]
    sums = (2, count // 2, height, lanes)
    return pl.pallas_call(
        functools.partial(
            final_body, block=block, per_part=per_part, extra=len(extra), outer=(row0 == 0, row0 + count == rows)
        ),
        grid_spec=pltpu.PrefetchScalarGridSpec(
            num_scalar_prefetch=1, grid=(2, per_part), in_specs=specs, out_specs=out_specs
        ),
        out_shape=[jax.ShapeDtypeStruct(shape, jnp.float32) for shape in (u.shape, sums, sums)],
        input_output_aliases=aliases,
        compiler_params=pltpu.CompilerParams(dimension_semantics=("arbitrary", "arbitrary")),
        name="finish",
    )(*operands)


def scale_body(bits, u, own, other, *refs, inverse):
    result = refs[-1]
    width = u.shape[1]

    def scaled(sums):
        def one_row(r, carry):
            mean = sums[0, 0, r] * inverse
            factor = lax.rsqrt(sums[0, 1, r] * inverse - mean * mean + 0.0001)
            mean = mean + 1.0
            for x in range(width):
                result[r, x] = (u[r, x] - mean) * factor
            return carry

        lax.fori_loop(0, u.shape[0], one_row, 0)

    @pl.when(pl.program_id(0) == 0)
    def _():
        scaled(own)

    @pl.when(pl.program_id(0) == 1)
    def _():
        scaled(other)


def scale(u, own, other, bits, row0, target, line_length):
    _, width, height, lanes = u.shape
    pieces, _, block = own.shape[:3]
    first = row0 // block

    def at(p, i, bits):
        return first + jnp.where(p == 0, bits[0], 1 - bits[0]) * pieces + (bits[1] ^ i if pieces > 1 else 0)

    full = pl.BlockSpec((block, width, height, lanes), lambda *g: (at(*g), 0, 0, 0))
    part = (1, 2, block, height, lanes)
    specs = [
        full,
        pl.BlockSpec(part, lambda p, i, m: (jnp.where(p == 0, i, pieces - 1), 0, 0, 0, 0)),
        pl.BlockSpec(part, lambda p, i, m: (jnp.where(p == 0, 0, i), 0, 0, 0, 0)),
    ]
    operands = [bits, u, own, other]
    aliases = {}
    if target is not None:
        aliases = {len(operands): 0}
        operands.append(target)
        specs.append(pl.BlockSpec(memory_space=pl.ANY))
    return pl.pallas_call(
        functools.partial(scale_body, inverse=1.0 / line_length),
        grid_spec=pltpu.PrefetchScalarGridSpec(num_scalar_prefetch=1, grid=(2, pieces), in_specs=specs, out_specs=full),
        out_shape=jax.ShapeDtypeStruct(u.shape, jnp.float32),
        input_output_aliases=aliases,
        compiler_params=pltpu.CompilerParams(dimension_semantics=("arbitrary", "arbitrary")),
        name="scale",
    )(*operands)


def body(u, k, s):
    rows, width, height, lanes = u.shape
    half, quarter = rows // 2, rows // 4
    place = lax.axis_index("px").astype(jnp.int32)
    column = place & 3
    right = column >> 1
    middle = (column ^ right) & 1
    by_near = jnp.stack([middle, right])
    by_far = jnp.stack([right, middle])

    x_halos = {row0: (exchange(pick(u, row0, half), "px"), half) for row0 in (0, half)}
    edges = by_parity("pz", u[:, :, 0].reshape(-1, lanes), u[:, :, height - 1].reshape(-1, lanes))
    z_halos = z_exchange(edges)
    y_low = (send_up(u[rows - 1 :], "py"), 0)
    y_high = (send_down(u[:1], "py"), 0)
    for step in range(1, STEPS):
        count = half if step < STEPS - 1 else quarter
        targets = ()
        arrived = {}
        for row0 in range(0, rows, count):
            received, length = x_halos[row0 // half * half]
            low = y_low if row0 == 0 else (u, row0 - 1)
            high = y_high if row0 + count == rows else (u, row0 + count)
            out = advance(u, (*received, *z_halos), low, high, k, s, row0, count, row0 % length, targets, 16)
            targets = out[:3]
            arrived[row0] = (exchange(out[3:5], "px"), count)
            if row0 == 0:
                next_high = (send_down(out[5], "py"), 0)
            if row0 + count == rows:
                next_low = (send_up(out[5], "py"), 0)
        u = targets[0]
        z_halos = z_exchange(targets[1:])
        x_halos, y_low, y_high = arrived, next_low, next_high

    def x_first(total, masks, bit):
        rows_left = total.shape[1] // 2
        part = lambda b: lax.dynamic_slice_in_dim(total, b * rows_left, rows_left, axis=1)
        total = part(bit) + swap(part(1 - bit), masks[1])
        total = total + swap(total, 4)
        total = jnp.stack([total, swap(total, masks[1])])
        return total, swap(total, masks[0])

    end = None
    sums = []
    for number, row0 in enumerate(range(0, rows, quarter)):
        masks, bits = ((3, 1), by_far) if number % 2 else ((1, 3), by_near)
        low = y_low if row0 == 0 else (u, row0 - 1)
        high = y_high if row0 + quarter == rows else (u, row0 + quarter)
        end, send, keep = finish(u, (*x_halos[row0][0], *z_halos), low, high, k, s, row0, quarter, 0, end, (), bits, 8)
        sums.append((*x_first(keep + swap(send, masks[0]), masks, bits[1]), bits))
    result = None
    for number, (own, other, bits) in enumerate(sums):
        result = scale(end, own, other, bits, number * quarter, result, width * lax.axis_size("px"))
    return result, end


def solution(mesh):
    placed = P("py", "px", "pz", None)
    return jax.shard_map(
        body, mesh=mesh, in_specs=(placed, placed, placed), out_specs=(placed, placed), check_vma=False
    )
```

```python
import functools

import jax
import jax.numpy as jnp
from jax import lax
from jax.experimental import pallas as pl
from jax.experimental.pallas import tpu as pltpu
from jax.sharding import PartitionSpec as P


STEPS = 4
GRANT = 4 * 2**20
ROUTES = ("over_near", "near", "far", "over_near")
SCALES = ((0, "both"), (2, "both"), (1, "both"), (3, "own"), (3, "other"))


def ring(value, axis, shift):
    devices = lax.axis_size(axis)
    return lax.ppermute(value, axis, [(i, (i + shift) % devices) for i in range(devices)])


def send_up(value, axis):
    return ring(value, axis, 1)


def send_down(value, axis):
    return ring(value, axis, -1)


def swap(value, mask):
    return lax.ppermute(value, "px", [(i, i ^ mask) for i in range(lax.axis_size("px"))])


def pair_swap(value, axis, odd):
    devices = lax.axis_size(axis)
    return lax.ppermute(value, axis, [(i, ((i - odd) ^ 1) + odd) for i in range(odd, devices - odd)])


def exchange(faces, axis):
    even = pair_swap(faces[0], axis, 0)
    odd = pair_swap(faces[1], axis, 1)
    return even, odd


def z_exchange(faces):
    last_x, last_z = lax.axis_size("px") - 1, lax.axis_size("pz") - 1
    flat = lambda x, z: x * (last_z + 1) + z
    direct = [(flat(x, a), flat(x, b)) for x in range(1, last_x) for a, b in ((1, 2), (2, 1))]
    out, back = [], []
    for x, over in ((0, last_x // 2 + 1), (last_x, last_x // 2)):
        out += [(flat(x, 1), flat(over, last_z)), (flat(x, 2), flat(over, 0))]
        back += [(flat(over, last_z), flat(x, 2)), (flat(over, 0), flat(x, 1))]
    even = pair_swap(faces[0], "pz", 0)
    odd = lax.ppermute(faces[1], ("px", "pz"), direct + out)
    over = lax.ppermute(odd, ("px", "pz"), back)
    return even, odd, over


def by_parity(axis, low, high):
    even = lax.axis_index(axis) % 2 == 0
    return jnp.where(even, high, low), jnp.where(even, low, high)


def inside(axis):
    at = lax.axis_index(axis)
    below = jnp.where(at > 0, 1.0, 0.0).astype(jnp.float32)
    above = jnp.where(at < lax.axis_size(axis) - 1, 1.0, 0.0).astype(jnp.float32)
    return below, above


def update_rows(refs, store, block, width, height, is_first, is_last, outer):
    u, before, after, low, high, xe, xo, ze, zo, zo_over, k, s = refs
    x_at, z_at = lax.axis_index("px"), lax.axis_index("pz")
    x_outer = (x_at == 0) | (x_at == lax.axis_size("px") - 1)
    z_inner = ((z_at > 0) & (z_at < lax.axis_size("pz") - 1)).astype(jnp.float32)
    x_even = lax.axis_index("px") % 2 == 0
    z_even = lax.axis_index("pz") % 2 == 0
    y_below, y_above = inside("py")
    sub = lax.broadcasted_iota(jnp.int32, (height, u.shape[-1]), 0)
    at_low = sub == 0
    at_high = sub == height - 1

    def one_row(r, below, above):
        for x in range(width):
            c = u[r, x]
            left = jnp.where(x_even, xo[r], xe[r]) if x == 0 else u[r, x - 1]
            right = jnp.where(x_even, xe[r], xo[r]) if x == width - 1 else u[r, x + 1]
            line = r * width + x
            z_first = ze[pl.ds(line, 1), :]
            z_second = jnp.where(x_outer, zo_over[pl.ds(line, 1), :], zo[pl.ds(line, 1), :]) * z_inner
            zd = jnp.where(at_low, jnp.where(z_even, z_second, z_first), pltpu.roll(c, 1, 0))
            zu = jnp.where(at_high, jnp.where(z_even, z_first, z_second), pltpu.roll(c, height - 1, 0))
            spread = below(x) + above(x) + left + right + zd + zu - 6.0 * c
            store(r, x, c + k[r, x] * spread + s[r, x])

    def lowest(x):
        return jnp.where(is_first, low[0, x] * y_below if outer[0] else low[0, x], before[0, x])

    def highest(x):
        return jnp.where(is_last, high[0, x] * y_above if outer[1] else high[0, x], after[0, x])

    one_row(0, lowest, lambda x: u[1, x])

    def middle(r, carry):
        one_row(r, lambda x: u[r - 1, x], lambda x: u[r + 1, x])
        return carry

    lax.fori_loop(1, block - 1, middle, 0)
    one_row(block - 1, lambda x: u[block - 2, x], highest)


def corner_body(right, middle, layer):
    at = lax.axis_index("px")
    column = at % 4
    right[0] = column // 2
    middle[0] = (column // 2 + column) % 2
    layer[0] = at // 4


def corner():
    bit = jax.ShapeDtypeStruct((1,), jnp.int32)
    return pl.pallas_call(
        corner_body,
        out_specs=[pl.BlockSpec(memory_space=pltpu.SMEM)] * 3,
        out_shape=[bit] * 3,
        compiler_params=pltpu.CompilerParams(vmem_limit_bytes=GRANT),
        name="corner",
    )()


def pick_body(low, high, even_face, odd_face):
    even_face[...], odd_face[...] = by_parity("px", low[:, 0], high[:, 0])


def pick(u, ranges, block):
    _, width, height, lanes = u.shape
    count = sum(length for _, length in ranges)
    position = positions(ranges, block)
    face = jax.ShapeDtypeStruct((count, height, lanes), jnp.float32)
    return pl.pallas_call(
        pick_body,
        grid=(count // block,),
        in_specs=[
            pl.BlockSpec((block, 1, height, lanes), lambda i: (position(i), 0, 0, 0)),
            pl.BlockSpec((block, 1, height, lanes), lambda i: (position(i), width - 1, 0, 0)),
        ],
        out_specs=[pl.BlockSpec((block, height, lanes), lambda i: (i, 0, 0))] * 2,
        out_shape=[face, face],
        compiler_params=pltpu.CompilerParams(dimension_semantics=("arbitrary",), vmem_limit_bytes=2 * GRANT),
        name="pick",
    )(u, u)


def step_body(*refs, block, position, last, extra, faces, outer):
    ins, outs = refs[:12], refs[12 + extra :]
    width, height = ins[0].shape[1:3]
    at = position(pl.program_id(0))
    kept = {}

    def store(r, x, value):
        outs[0][r, x] = value
        if x == 0:
            kept["low"] = value
        if x == width - 1:
            outs[3][r], outs[4][r] = by_parity("px", kept["low"], value)
        line = pl.ds(r * width + x, 1)
        outs[1][line, :], outs[2][line, :] = by_parity("pz", value[0:1], value[height - 1 : height])

    update_rows(ins, store, block, width, height, at == 0, at == last, outer)
    for face, (edge, row) in zip(outs[5:], faces):

        @pl.when(at == edge)
        def _(face=face, row=row):
            face[0] = outs[0][row]


def positions(ranges, block):
    def position(i):
        at, done = ranges[0][0] // block + i, ranges[0][1] // block
        for start, count in ranges[1:]:
            at = jnp.where(i < done, at, start // block + i - done)
            done += count // block
        return at

    return position


def field_specs(position, offset, rows, block, width, height, lanes, place):
    full = (block, width, height, lanes)
    one = (1, width, height, lanes)
    extra = offset // block
    at = lambda *g: position(place(*g))
    face = pl.BlockSpec((block, height, lanes), lambda *g: (extra + place(*g), 0, 0))
    edge = pl.BlockSpec((block * width, lanes), lambda *g: (at(*g), 0))
    return [
        pl.BlockSpec(full, lambda *g: (at(*g), 0, 0, 0)),
        pl.BlockSpec(one, lambda *g: (jnp.maximum(at(*g) * block - 1, 0), 0, 0, 0)),
        pl.BlockSpec(one, lambda *g: (jnp.minimum((at(*g) + 1) * block, rows - 1), 0, 0, 0)),
        pl.BlockSpec(one, lambda *g: (0, 0, 0, 0)),
        pl.BlockSpec(one, lambda *g: (0, 0, 0, 0)),
        face,
        face,
        edge,
        edge,
        edge,
        pl.BlockSpec(full, lambda *g: (at(*g), 0, 0, 0)),
        pl.BlockSpec(full, lambda *g: (at(*g), 0, 0, 0)),
    ]


def advance(u, halos, low, high, k, s, ranges, offset, targets, block):
    rows, width, height, lanes = u.shape
    count = sum(length for _, length in ranges)
    block = min(block, count)
    position = positions(ranges, block)
    last = rows // block - 1
    specs = field_specs(position, offset, rows, block, width, height, lanes, lambda i: i)
    operands = [u, u, u, low, high, *halos, k, s]
    aliases = {}
    for number, target in enumerate(targets):
        aliases[len(operands)] = number
        operands.append(target)
        specs.append(pl.BlockSpec(memory_space=pl.ANY))
    face = pl.BlockSpec((block, height, lanes), lambda i: (i, 0, 0))
    edge = pl.BlockSpec((block * width, lanes), lambda i: (position(i), 0))
    out_specs = [pl.BlockSpec((block, width, height, lanes), lambda i: (position(i), 0, 0, 0)), edge, edge, face, face]
    shapes = [u.shape] + [(rows * width, lanes)] * 2 + [(count, height, lanes)] * 2
    outer = (ranges[0][0] == 0, sum(ranges[-1]) == rows)
    faces = [(0, 0)] * outer[0] + [(last, block - 1)] * outer[1]
    out_specs += [pl.BlockSpec((1, width, height, lanes), lambda i: (0, 0, 0, 0))] * len(faces)
    shapes += [(1, width, height, lanes)] * len(faces)
    return pl.pallas_call(
        functools.partial(
            step_body, block=block, position=position, last=last, extra=len(targets), faces=faces, outer=outer
        ),
        grid=(count // block,),
        in_specs=specs,
        out_specs=out_specs,
        out_shape=[jax.ShapeDtypeStruct(shape, jnp.float32) for shape in shapes],
        input_output_aliases=aliases,
        compiler_params=pltpu.CompilerParams(dimension_semantics=("arbitrary",), vmem_limit_bytes=GRANT),
        name="advance",
    )(*operands)


def final_body(bit, *refs, block, per_part, position, last, extra, outer):
    ins, outs = refs[:12], refs[12 + extra :]
    width, height = ins[0].shape[1:3]
    p, i = pl.program_id(0), pl.program_id(1)
    at = position(jnp.where(p == 0, 1 - bit[0], bit[0]) * per_part + i)
    result, send, keep = outs
    totals = {}

    def stats_to(target):
        def store(r, x, value):
            result[r, x] = value
            moved = value - 1.0
            totals["sum"] = moved if x == 0 else totals["sum"] + moved
            totals["square"] = moved * moved if x == 0 else totals["square"] + moved * moved
            if x == width - 1:
                target[0, r] = totals["sum"]
                target[1, r] = totals["square"]

        update_rows(ins, store, block, width, height, at == 0, at == last, outer)

    @pl.when(p == 0)
    def _():
        stats_to(send)

    @pl.when(p == 1)
    def _():
        stats_to(keep)


def finish(u, halos, low, high, k, s, row0, count, target, bit, block):
    rows, width, height, lanes = u.shape
    block = min(block, count // 2)
    per_part = count // 2 // block
    position = positions([(row0, count)], block)

    def place(p, i, bit):
        return jnp.where(p == 0, 1 - bit[0], bit[0]) * per_part + i

    specs = field_specs(position, 0, rows, block, width, height, lanes, place)
    operands = [bit, u, u, u, low, high, *halos, k, s]
    aliases = {}
    if target is not None:
        aliases = {len(operands): 0}
        operands.append(target)
        specs.append(pl.BlockSpec(memory_space=pl.ANY))
    part = (2, block, height, lanes)
    out_specs = [
        pl.BlockSpec((block, width, height, lanes), lambda *g: (position(place(*g)), 0, 0, 0)),
        pl.BlockSpec(part, lambda p, i, m: (0, jnp.where(p == 0, i, per_part - 1), 0, 0)),
        pl.BlockSpec(part, lambda p, i, m: (0, jnp.where(p == 0, 0, i), 0, 0)),
    ]
    sums = (2, count // 2, height, lanes)
    return pl.pallas_call(
        functools.partial(
            final_body,
            block=block,
            per_part=per_part,
            position=position,
            last=rows // block - 1,
            extra=len(aliases),
            outer=(row0 == 0, row0 + count == rows),
        ),
        grid_spec=pltpu.PrefetchScalarGridSpec(
            num_scalar_prefetch=1, grid=(2, per_part), in_specs=specs, out_specs=out_specs
        ),
        out_shape=[jax.ShapeDtypeStruct(shape, jnp.float32) for shape in (u.shape, sums, sums)],
        input_output_aliases=aliases,
        compiler_params=pltpu.CompilerParams(
            dimension_semantics=("arbitrary", "arbitrary"), vmem_limit_bytes=GRANT
        ),
        name="finish",
    )(*operands)


def fold_body(bit, keep, came, mine, theirs):
    for half in range(2):
        total = keep[:, half] + came[:, half]

        @pl.when(half == bit[0])
        def _(total=total):
            mine[...] = total

        @pl.when(half != bit[0])
        def _(total=total):
            theirs[...] = total


def fold(keep, came, bit):
    _, rows, height, lanes = keep.shape
    cut = (2, 2, rows // 2, height, lanes)
    half = (2, rows // 2, height, lanes)
    return pl.pallas_call(
        fold_body,
        in_specs=[pl.BlockSpec(memory_space=pltpu.SMEM)] + [pl.BlockSpec(cut, lambda: (0,) * 5)] * 2,
        out_specs=[pl.BlockSpec(half, lambda: (0,) * 4)] * 2,
        out_shape=[jax.ShapeDtypeStruct(half, jnp.float32)] * 2,
        compiler_params=pltpu.CompilerParams(vmem_limit_bytes=GRANT),
        name="fold",
    )(bit, keep.reshape(cut), came.reshape(cut))


def scale_body(bit, piece_bit, u, *refs, parts, inverse):
    result = refs[-1]
    width = u.shape[1]

    def scaled(sums):
        def one_row(r, carry):
            mean = sums[0, 0, r] * inverse
            factor = lax.rsqrt(sums[0, 1, r] * inverse - mean * mean + 0.0001)
            mean = mean + 1.0
            for x in range(width):
                result[r, x] = (u[r, x] - mean) * factor
            return carry

        lax.fori_loop(0, u.shape[0], one_row, 0)

    for number, sums in enumerate(refs[:parts]):

        @pl.when(pl.program_id(0) == number)
        def _(sums=sums):
            scaled(sums)


def scale(u, halves, flips, bits, row0, target, line_length):
    _, width, height, lanes = u.shape
    pieces, _, block = halves[0].shape[:3]
    first = row0 // block

    def at(p, i, bit, piece_bit):
        flip = jnp.where(p == 0, flips[0], flips[-1])
        return first + (bit[0] ^ flip) * pieces + (piece_bit[0] ^ i)

    full = pl.BlockSpec((block, width, height, lanes), lambda *g: (at(*g), 0, 0, 0))
    part = (1, 2, block, height, lanes)
    specs = [full]
    for number in range(len(halves)):
        specs.append(
            pl.BlockSpec(
                part,
                lambda p, i, *m, number=number: (
                    jnp.where(p == number, i, jnp.where(p < number, 0, pieces - 1)), 0, 0, 0, 0
                ),
            )
        )
    operands = [*bits, u, *halves]
    aliases = {}
    if target is not None:
        aliases = {len(operands): 0}
        operands.append(target)
        specs.append(pl.BlockSpec(memory_space=pl.ANY))
    return pl.pallas_call(
        functools.partial(scale_body, parts=len(halves), inverse=1.0 / line_length),
        grid_spec=pltpu.PrefetchScalarGridSpec(
            num_scalar_prefetch=2, grid=(len(halves), pieces), in_specs=specs, out_specs=full
        ),
        out_shape=jax.ShapeDtypeStruct(u.shape, jnp.float32),
        input_output_aliases=aliases,
        compiler_params=pltpu.CompilerParams(
            dimension_semantics=("arbitrary", "arbitrary"), vmem_limit_bytes=GRANT
        ),
        name="scale",
    )(*operands)


def body(u, k, s):
    rows, width, height, lanes = u.shape
    half, quarter = rows // 2, rows // 4
    right, middle, layer = corner()
    routes = {
        "near": (1, 3, 4, (middle, right)),
        "far": (3, 1, 4, (right, middle)),
        "over_near": (4, 1, 3, (layer, middle)),
        "over_far": (4, 3, 1, (layer, right)),
    }

    inner = [(quarter, half)]
    outer = [(0, quarter), (rows - quarter, quarter)]
    quarters = [(quarter, quarter), (half, quarter), (0, quarter), (rows - quarter, quarter)]

    start = pltpu.with_memory_space_constraint(u, pltpu.HBM)
    x_halos = [exchange(pick(start, inner, quarter), "px"), exchange(pick(start, outer, quarter), "px")]
    z_halos = z_exchange(by_parity("pz", u[:, :, 0].reshape(-1, lanes), u[:, :, height - 1].reshape(-1, lanes)))
    y_low = send_up(u[rows - 1 :], "py")
    y_high = send_down(u[:1], "py")
    for step in range(1, STEPS):
        targets = ()
        arrived, borders = [], []
        chunks = [inner, outer] if step < STEPS - 1 else [[part] for part in quarters]
        for number, ranges in enumerate(chunks):
            received = x_halos[number * 2 // len(chunks)]
            offset = number % 2 * quarter if len(chunks) == 4 else 0
            low, high = (y_low, y_high) if number >= len(chunks) // 2 else (u, u)
            number = number * 4 // len(chunks)
            out = advance(u, (*received, *z_halos), low, high, k, s, ranges, offset, targets, 16)
            targets = out[:3]
            arrived.append(exchange(out[3:5], "px"))
            borders += out[5:]
        u = targets[0]
        z_halos = z_exchange(targets[1:])
        y_high = send_down(borders[0], "py")
        y_low = send_up(borders[1], "py")
        x_halos = arrived

    def line_sums(send, keep, route):
        outer_mask, inner_mask, last_mask, bits = route
        mine, theirs = fold(keep, swap(send, outer_mask), bits[1])
        total = mine + swap(theirs, inner_mask)
        total = total + swap(total, last_mask)
        total = jnp.stack([total, swap(total, inner_mask)])
        return total, swap(total, outer_mask), bits

    end = None
    sums = []
    for number, (row0, count) in enumerate(quarters):
        route = routes[ROUTES[number]]
        low, high = (y_low, y_high) if number >= 2 else (u, u)
        end, send, keep = finish(u, (*x_halos[number], *z_halos), low, high, k, s, row0, count, end, route[3][0], 8)
        sums.append(line_sums(send, keep, route))
    result = None
    for number, wanted in SCALES:
        own, other, bits = sums[number]
        halves = {"both": ((own, other), (0, 1)), "own": ((own,), (0,)), "other": ((other,), (1,))}[wanted]
        result = scale(end, *halves, bits, quarters[number][0], result, width * lax.axis_size("px"))
    return result, end


def solution(mesh):
    placed = P("py", "px", "pz", None)
    return jax.shard_map(
        body, mesh=mesh, in_specs=(placed, placed, placed), out_specs=(placed, placed), check_vma=False
    )
```

```python
import functools

import jax
import jax.numpy as jnp
from jax import lax
from jax.experimental import pallas as pl
from jax.experimental.pallas import tpu as pltpu
from jax.sharding import PartitionSpec as P


STEPS = 4
GRANT = 4 * 2**20
ROUTES = ("over_near", "near", "far", "over_near")
SCALES = ((0, "own"), (2, "own"), (0, "other"), (3, "own"), (2, "other"), (1, "both"), (3, "other"))


def ring(value, axis, shift):
    devices = lax.axis_size(axis)
    return lax.ppermute(value, axis, [(i, (i + shift) % devices) for i in range(devices)])


def send_up(value, axis):
    return ring(value, axis, 1)


def send_down(value, axis):
    return ring(value, axis, -1)


def swap(value, mask):
    return lax.ppermute(value, "px", [(i, i ^ mask) for i in range(lax.axis_size("px"))])


def pair_swap(value, axis, odd):
    devices = lax.axis_size(axis)
    return lax.ppermute(value, axis, [(i, ((i - odd) ^ 1) + odd) for i in range(odd, devices - odd)])


def exchange(faces, axis):
    even = pair_swap(faces[0], axis, 0)
    odd = pair_swap(faces[1], axis, 1)
    return even, odd


def z_exchange(faces):
    last_x, last_z = lax.axis_size("px") - 1, lax.axis_size("pz") - 1
    flat = lambda x, z: x * (last_z + 1) + z
    direct = [(flat(x, a), flat(x, b)) for x in range(1, last_x) for a, b in ((1, 2), (2, 1))]
    out, back = [], []
    for x, over in ((0, last_x // 2 + 1), (last_x, last_x // 2)):
        out += [(flat(x, 1), flat(over, last_z)), (flat(x, 2), flat(over, 0))]
        back += [(flat(over, last_z), flat(x, 2)), (flat(over, 0), flat(x, 1))]
    even = pair_swap(faces[0], "pz", 0)
    odd = lax.ppermute(faces[1], ("px", "pz"), direct + out)
    over = lax.ppermute(odd, ("px", "pz"), back)
    return even, odd, over


def by_parity(axis, low, high):
    even = lax.axis_index(axis) % 2 == 0
    return jnp.where(even, high, low), jnp.where(even, low, high)


def inside(axis):
    at = lax.axis_index(axis)
    below = jnp.where(at > 0, 1.0, 0.0).astype(jnp.float32)
    above = jnp.where(at < lax.axis_size(axis) - 1, 1.0, 0.0).astype(jnp.float32)
    return below, above


def update_rows(refs, store, block, width, height, is_first, is_last, outer):
    u, before, after, low, high, xe, xo, ze, zo, zo_over, k, s = refs
    x_at, z_at = lax.axis_index("px"), lax.axis_index("pz")
    x_outer = (x_at == 0) | (x_at == lax.axis_size("px") - 1)
    z_inner = ((z_at > 0) & (z_at < lax.axis_size("pz") - 1)).astype(jnp.float32)
    x_even = lax.axis_index("px") % 2 == 0
    z_even = lax.axis_index("pz") % 2 == 0
    y_below, y_above = inside("py")
    sub = lax.broadcasted_iota(jnp.int32, (height, u.shape[-1]), 0)
    at_low = sub == 0
    at_high = sub == height - 1

    def one_row(r, below, above):
        for x in range(width):
            c = u[r, x]
            left = jnp.where(x_even, xo[r], xe[r]) if x == 0 else u[r, x - 1]
            right = jnp.where(x_even, xe[r], xo[r]) if x == width - 1 else u[r, x + 1]
            line = r * width + x
            z_first = ze[pl.ds(line, 1), :]
            z_second = jnp.where(x_outer, zo_over[pl.ds(line, 1), :], zo[pl.ds(line, 1), :]) * z_inner
            zd = jnp.where(at_low, jnp.where(z_even, z_second, z_first), pltpu.roll(c, 1, 0))
            zu = jnp.where(at_high, jnp.where(z_even, z_first, z_second), pltpu.roll(c, height - 1, 0))
            spread = below(x) + above(x) + left + right + zd + zu - 6.0 * c
            store(r, x, c + k[r, x] * spread + s[r, x])

    def lowest(x):
        return jnp.where(is_first, low[0, x] * y_below if outer[0] else low[0, x], before[0, x])

    def highest(x):
        return jnp.where(is_last, high[0, x] * y_above if outer[1] else high[0, x], after[0, x])

    one_row(0, lowest, lambda x: u[1, x])

    def middle(r, carry):
        one_row(r, lambda x: u[r - 1, x], lambda x: u[r + 1, x])
        return carry

    lax.fori_loop(1, block - 1, middle, 0)
    one_row(block - 1, lambda x: u[block - 2, x], highest)


def corner_body(right, middle, layer):
    at = lax.axis_index("px")
    column = at % 4
    right[0] = column // 2
    middle[0] = (column // 2 + column) % 2
    layer[0] = at // 4


def corner():
    bit = jax.ShapeDtypeStruct((1,), jnp.int32)
    return pl.pallas_call(
        corner_body,
        out_specs=[pl.BlockSpec(memory_space=pltpu.SMEM)] * 3,
        out_shape=[bit] * 3,
        compiler_params=pltpu.CompilerParams(vmem_limit_bytes=GRANT),
        name="corner",
    )()


def pick_body(low, high, even_face, odd_face):
    even_face[...], odd_face[...] = by_parity("px", low[:, 0], high[:, 0])


def pick(u, ranges, block):
    _, width, height, lanes = u.shape
    count = sum(length for _, length in ranges)
    position = positions(ranges, block)
    face = jax.ShapeDtypeStruct((count, height, lanes), jnp.float32)
    return pl.pallas_call(
        pick_body,
        grid=(count // block,),
        in_specs=[
            pl.BlockSpec((block, 1, height, lanes), lambda i: (position(i), 0, 0, 0)),
            pl.BlockSpec((block, 1, height, lanes), lambda i: (position(i), width - 1, 0, 0)),
        ],
        out_specs=[pl.BlockSpec((block, height, lanes), lambda i: (i, 0, 0))] * 2,
        out_shape=[face, face],
        compiler_params=pltpu.CompilerParams(dimension_semantics=("arbitrary",), vmem_limit_bytes=2 * GRANT),
        name="pick",
    )(u, u)


def step_body(*refs, block, position, last, extra, faces, outer):
    ins, outs = refs[:12], refs[12 + extra :]
    width, height = ins[0].shape[1:3]
    at = position(pl.program_id(0))
    kept = {}

    def store(r, x, value):
        outs[0][r, x] = value
        if x == 0:
            kept["low"] = value
        if x == width - 1:
            outs[3][r], outs[4][r] = by_parity("px", kept["low"], value)
        line = pl.ds(r * width + x, 1)
        outs[1][line, :], outs[2][line, :] = by_parity("pz", value[0:1], value[height - 1 : height])

    update_rows(ins, store, block, width, height, at == 0, at == last, outer)
    for face, (edge, row) in zip(outs[5:], faces):

        @pl.when(at == edge)
        def _(face=face, row=row):
            face[0] = outs[0][row]


def positions(ranges, block):
    def position(i):
        at, done = ranges[0][0] // block + i, ranges[0][1] // block
        for start, count in ranges[1:]:
            at = jnp.where(i < done, at, start // block + i - done)
            done += count // block
        return at

    return position


def field_specs(position, offset, rows, block, width, height, lanes, place):
    full = (block, width, height, lanes)
    one = (1, width, height, lanes)
    extra = offset // block
    at = lambda *g: position(place(*g))
    face = pl.BlockSpec((block, height, lanes), lambda *g: (extra + place(*g), 0, 0))
    edge = pl.BlockSpec((block * width, lanes), lambda *g: (at(*g), 0))
    return [
        pl.BlockSpec(full, lambda *g: (at(*g), 0, 0, 0)),
        pl.BlockSpec(one, lambda *g: (jnp.maximum(at(*g) * block - 1, 0), 0, 0, 0)),
        pl.BlockSpec(one, lambda *g: (jnp.minimum((at(*g) + 1) * block, rows - 1), 0, 0, 0)),
        pl.BlockSpec(one, lambda *g: (0, 0, 0, 0)),
        pl.BlockSpec(one, lambda *g: (0, 0, 0, 0)),
        face,
        face,
        edge,
        edge,
        edge,
        pl.BlockSpec(full, lambda *g: (at(*g), 0, 0, 0)),
        pl.BlockSpec(full, lambda *g: (at(*g), 0, 0, 0)),
    ]


def advance(u, halos, low, high, k, s, ranges, offset, targets, block):
    rows, width, height, lanes = u.shape
    count = sum(length for _, length in ranges)
    block = min(block, count)
    position = positions(ranges, block)
    last = rows // block - 1
    specs = field_specs(position, offset, rows, block, width, height, lanes, lambda i: i)
    operands = [u, u, u, low, high, *halos, k, s]
    aliases = {}
    for number, target in enumerate(targets):
        aliases[len(operands)] = number
        operands.append(target)
        specs.append(pl.BlockSpec(memory_space=pl.ANY))
    face = pl.BlockSpec((block, height, lanes), lambda i: (i, 0, 0))
    edge = pl.BlockSpec((block * width, lanes), lambda i: (position(i), 0))
    out_specs = [pl.BlockSpec((block, width, height, lanes), lambda i: (position(i), 0, 0, 0)), edge, edge, face, face]
    shapes = [u.shape] + [(rows * width, lanes)] * 2 + [(count, height, lanes)] * 2
    outer = (ranges[0][0] == 0, sum(ranges[-1]) == rows)
    faces = [(0, 0)] * outer[0] + [(last, block - 1)] * outer[1]
    out_specs += [pl.BlockSpec((1, width, height, lanes), lambda i: (0, 0, 0, 0))] * len(faces)
    shapes += [(1, width, height, lanes)] * len(faces)
    return pl.pallas_call(
        functools.partial(
            step_body, block=block, position=position, last=last, extra=len(targets), faces=faces, outer=outer
        ),
        grid=(count // block,),
        in_specs=specs,
        out_specs=out_specs,
        out_shape=[jax.ShapeDtypeStruct(shape, jnp.float32) for shape in shapes],
        input_output_aliases=aliases,
        compiler_params=pltpu.CompilerParams(dimension_semantics=("arbitrary",), vmem_limit_bytes=GRANT),
        name="advance",
    )(*operands)


def final_body(bit, *refs, block, per_part, position, last, extra, outer):
    ins, outs = refs[:12], refs[12 + extra :]
    width, height = ins[0].shape[1:3]
    p, i = pl.program_id(0), pl.program_id(1)
    at = position(jnp.where(p == 0, 1 - bit[0], bit[0]) * per_part + i)
    result, send, keep = outs
    totals = {}

    def stats_to(target):
        def store(r, x, value):
            result[r, x] = value
            moved = value - 1.0
            totals["sum"] = moved if x == 0 else totals["sum"] + moved
            totals["square"] = moved * moved if x == 0 else totals["square"] + moved * moved
            if x == width - 1:
                target[0, r] = totals["sum"]
                target[1, r] = totals["square"]

        update_rows(ins, store, block, width, height, at == 0, at == last, outer)

    @pl.when(p == 0)
    def _():
        stats_to(send)

    @pl.when(p == 1)
    def _():
        stats_to(keep)


def finish(u, halos, low, high, k, s, row0, count, target, bit, block):
    rows, width, height, lanes = u.shape
    block = min(block, count // 2)
    per_part = count // 2 // block
    position = positions([(row0, count)], block)

    def place(p, i, bit):
        return jnp.where(p == 0, 1 - bit[0], bit[0]) * per_part + i

    specs = field_specs(position, 0, rows, block, width, height, lanes, place)
    operands = [bit, u, u, u, low, high, *halos, k, s]
    aliases = {}
    if target is not None:
        aliases = {len(operands): 0}
        operands.append(target)
        specs.append(pl.BlockSpec(memory_space=pl.ANY))
    part = (2, block, height, lanes)
    out_specs = [
        pl.BlockSpec((block, width, height, lanes), lambda *g: (position(place(*g)), 0, 0, 0)),
        pl.BlockSpec(part, lambda p, i, m: (0, jnp.where(p == 0, i, per_part - 1), 0, 0)),
        pl.BlockSpec(part, lambda p, i, m: (0, jnp.where(p == 0, 0, i), 0, 0)),
    ]
    sums = (2, count // 2, height, lanes)
    return pl.pallas_call(
        functools.partial(
            final_body,
            block=block,
            per_part=per_part,
            position=position,
            last=rows // block - 1,
            extra=len(aliases),
            outer=(row0 == 0, row0 + count == rows),
        ),
        grid_spec=pltpu.PrefetchScalarGridSpec(
            num_scalar_prefetch=1, grid=(2, per_part), in_specs=specs, out_specs=out_specs
        ),
        out_shape=[jax.ShapeDtypeStruct(shape, jnp.float32) for shape in (u.shape, sums, sums)],
        input_output_aliases=aliases,
        compiler_params=pltpu.CompilerParams(
            dimension_semantics=("arbitrary", "arbitrary"), vmem_limit_bytes=GRANT
        ),
        name="finish",
    )(*operands)


def fold_body(bit, keep, came, mine, theirs):
    for half in range(2):
        total = keep[:, half] + came[:, half]

        @pl.when(half == bit[0])
        def _(total=total):
            mine[...] = total

        @pl.when(half != bit[0])
        def _(total=total):
            theirs[...] = total


def fold(keep, came, bit):
    _, rows, height, lanes = keep.shape
    cut = (2, 2, rows // 2, height, lanes)
    half = (2, rows // 2, height, lanes)
    return pl.pallas_call(
        fold_body,
        in_specs=[pl.BlockSpec(memory_space=pltpu.SMEM)] + [pl.BlockSpec(cut, lambda: (0,) * 5)] * 2,
        out_specs=[pl.BlockSpec(half, lambda: (0,) * 4)] * 2,
        out_shape=[jax.ShapeDtypeStruct(half, jnp.float32)] * 2,
        compiler_params=pltpu.CompilerParams(vmem_limit_bytes=GRANT),
        name="fold",
    )(bit, keep.reshape(cut), came.reshape(cut))


def scale_body(bit, piece_bit, u, *refs, parts, inverse):
    result = refs[-1]
    width = u.shape[1]

    def scaled(sums):
        def one_row(r, carry):
            mean = sums[0, 0, r] * inverse
            factor = lax.rsqrt(sums[0, 1, r] * inverse - mean * mean + 0.0001)
            mean = mean + 1.0
            for x in range(width):
                result[r, x] = (u[r, x] - mean) * factor
            return carry

        lax.fori_loop(0, u.shape[0], one_row, 0)

    for number, sums in enumerate(refs[:parts]):

        @pl.when(pl.program_id(0) == number)
        def _(sums=sums):
            scaled(sums)


def scale(u, halves, flips, bits, row0, target, line_length):
    _, width, height, lanes = u.shape
    pieces, _, block = halves[0].shape[:3]
    first = row0 // block

    def at(p, i, bit, piece_bit):
        flip = jnp.where(p == 0, flips[0], flips[-1])
        return first + (bit[0] ^ flip) * pieces + (piece_bit[0] ^ i)

    full = pl.BlockSpec((block, width, height, lanes), lambda *g: (at(*g), 0, 0, 0))
    part = (1, 2, block, height, lanes)
    specs = [full]
    for number in range(len(halves)):
        specs.append(
            pl.BlockSpec(
                part,
                lambda p, i, *m, number=number: (
                    jnp.where(p == number, i, jnp.where(p < number, 0, pieces - 1)), 0, 0, 0, 0
                ),
            )
        )
    operands = [*bits, u, *halves]
    aliases = {}
    if target is not None:
        aliases = {len(operands): 0}
        operands.append(target)
        specs.append(pl.BlockSpec(memory_space=pl.ANY))
    return pl.pallas_call(
        functools.partial(scale_body, parts=len(halves), inverse=1.0 / line_length),
        grid_spec=pltpu.PrefetchScalarGridSpec(
            num_scalar_prefetch=2, grid=(len(halves), pieces), in_specs=specs, out_specs=full
        ),
        out_shape=jax.ShapeDtypeStruct(u.shape, jnp.float32),
        input_output_aliases=aliases,
        compiler_params=pltpu.CompilerParams(
            dimension_semantics=("arbitrary", "arbitrary"), vmem_limit_bytes=GRANT
        ),
        name="scale",
    )(*operands)


def body(u, k, s):
    rows, width, height, lanes = u.shape
    half, quarter = rows // 2, rows // 4
    right, middle, layer = corner()
    routes = {
        "near": (1, 3, 4, (middle, right)),
        "far": (3, 1, 4, (right, middle)),
        "over_near": (4, 1, 3, (layer, middle)),
        "over_far": (4, 3, 1, (layer, right)),
    }

    inner = [(quarter, half)]
    outer = [(0, quarter), (rows - quarter, quarter)]
    quarters = [(quarter, quarter), (half, quarter), (0, quarter), (rows - quarter, quarter)]

    start = pltpu.with_memory_space_constraint(u, pltpu.HBM)
    x_halos = [exchange(pick(start, inner, quarter), "px"), exchange(pick(start, outer, quarter), "px")]
    z_halos = z_exchange(by_parity("pz", u[:, :, 0].reshape(-1, lanes), u[:, :, height - 1].reshape(-1, lanes)))
    y_low = send_up(u[rows - 1 :], "py")
    y_high = send_down(u[:1], "py")
    for step in range(1, STEPS):
        targets = ()
        arrived, borders = [], []
        chunks = [inner, outer] if step < STEPS - 1 else [[part] for part in quarters]
        for number, ranges in enumerate(chunks):
            received = x_halos[number * 2 // len(chunks)]
            offset = number % 2 * quarter if len(chunks) == 4 else 0
            low, high = (y_low, y_high) if number >= len(chunks) // 2 else (u, u)
            number = number * 4 // len(chunks)
            out = advance(u, (*received, *z_halos), low, high, k, s, ranges, offset, targets, 32)
            targets = out[:3]
            arrived.append(exchange(out[3:5], "px"))
            borders += out[5:]
        u = targets[0]
        z_halos = z_exchange(targets[1:])
        y_high = send_down(borders[0], "py")
        y_low = send_up(borders[1], "py")
        x_halos = arrived

    def line_sums(send, keep, route):
        outer_mask, inner_mask, last_mask, bits = route
        mine, theirs = fold(keep, swap(send, outer_mask), bits[1])
        total = mine + swap(theirs, inner_mask)
        total = total + swap(total, last_mask)
        total = jnp.stack([total, swap(total, inner_mask)])
        return total, swap(total, outer_mask), bits

    end = None
    sums = []
    for number, (row0, count) in enumerate(quarters):
        route = routes[ROUTES[number]]
        low, high = (y_low, y_high) if number >= 2 else (u, u)
        end, send, keep = finish(u, (*x_halos[number], *z_halos), low, high, k, s, row0, count, end, route[3][0], 16)
        sums.append(line_sums(send, keep, route))
    result = None
    for number, wanted in SCALES:
        own, other, bits = sums[number]
        halves = {"both": ((own, other), (0, 1)), "own": ((own,), (0,)), "other": ((other,), (1,))}[wanted]
        result = scale(end, *halves, bits, quarters[number][0], result, width * lax.axis_size("px"))
    return result, end


def solution(mesh):
    placed = P("py", "px", "pz", None)
    return jax.shard_map(
        body, mesh=mesh, in_specs=(placed, placed, placed), out_specs=(placed, placed), check_vma=False
    )
```
